256 devices in a mesh: dp: 8 (over y, core), expert: 32 (over x, z).
Axes of the slice: x: 4, y: 4, z: 8, core: 2. Of those that a mesh axis runs over, the one named last changes fastest.
Arguments:
- tokens: bfloat16 [4096, 4096], P(('dp', 'expert')), may hold values from -6 to 6
- expert_ids: int32 [4096, 2], P(('dp', 'expert')), may hold values from 0 to 7, all different within a row; in each aligned block of 16 rows (0 to 15, 16 to 31, ...) at most 6 rows name the same one
- gate_quota: int32 [4096, 2], P(('dp', 'expert')), may hold values from 1 to 32767
- w_gate: bfloat16 [32, 4096, 2048], P('expert', None, 'dp'), may hold values from -0.09375 to 0.09375
- w_up: bfloat16 [32, 4096, 2048], P('expert', None, 'dp'), may hold values from -0.09375 to 0.09375
- w_down: bfloat16 [32, 2048, 4096], P('expert', 'dp'), may hold values from -0.0625 to 0.0625
Outputs:
- mixed_out: bfloat16 [4096, 4096], P(('dp', 'expert'))
The draws below stay inside these ranges and needn't reach their ends.
Inputs may be any that keep to these rules, and one draw needn't show every extreme that they name: `expert_ids`: each row names 2 different experts; among the rows of one device no expert is named more than 6 times.
All inputs are finite; a program needn't handle non-finite values.
Results may differ from the reference program's by a relative error of at most 0.015.
Values may be sent and summed in bfloat16 or wider, within the bound.
No kernel may reach another device: no remote copies, remote signals or barrier semaphores. Data moves between devices by JAX's collectives and lax.ppermute only.
A program may use at most 128 MiB of HBM per device.

```python
import math
import jax
import jax.numpy as jnp
import numpy as np
from jax import lax

D = 4096
FF = 8192
EXPERTS = 8
TOP = 2
TOK_DEV = 16
CAP = 6
GROUP = 4
TOKENS = 4096
N_DP = 8
N_EXPERT = 32


def set_ends(array, stream_key, least, largest):
    spot = [jax.random.randint(jax.random.fold_in(stream_key, axis), (), 0, length) for axis, length in enumerate(array.shape)]
    widest = array.shape.index(max(array.shape))
    next_to = spot[:widest] + [(spot[widest] + 1) % array.shape[widest]] + spot[widest + 1:]
    return array.at[tuple(spot)].set(least).at[tuple(next_to)].set(largest)


def level_of(own_key, shape, shards, least, largest):
    gain = 1.0
    for axis_at, parts in shards:
        steps = jax.random.uniform(jax.random.fold_in(jax.random.fold_in(own_key, 6), axis_at), (parts,), jnp.float32, least / len(shards), largest / len(shards))
        gain = gain * jnp.repeat(jnp.exp(steps), shape[axis_at] // parts).reshape((-1,) + (1,) * (len(shape) - 1 - axis_at))
    return gain


def assign_block(stream_key, own, number, rows, amount, top, reach, slope):
    order = jax.random.permutation(stream_key, amount)
    heavy_load, common = load_shares(amount, rows * top, reach, slope, True), load_shares(amount, rows * top, reach, slope, False)
    places = jnp.arange(amount)

    def named(tallies, offset_by):
        used = int((tallies > 0).sum())
        fixed = max(1, used // 4)
        moved = fixed + (places - fixed + offset_by * (used - fixed)) % max(1, amount - fixed)
        return jnp.zeros((amount,), jnp.int32).at[order[jnp.where(places < fixed, places, moved)]].set(jnp.asarray(tallies, jnp.int32))

    tallies = jnp.where(number % 4 == 0, named(heavy_load, number // 4), named(common, number - number // 4 - 1))
    mixed = jax.random.permutation(jax.random.fold_in(own, 3), amount)
    giver, sink = mixed[0:amount // 2 * 2:2], mixed[1:amount // 2 * 2:2]
    room = jnp.minimum(tallies[giver] - 1, reach - tallies[sink]) // 2
    room = jnp.where((giver == order[0]) | (sink == order[0]) | (tallies[sink] == 0), 0, jnp.maximum(room, 0))
    moved = jax.random.randint(jax.random.fold_in(own, 4), (amount // 2,), 0, 1 << 20) % (room + 1)
    tallies = tallies.at[giver].add(-moved).at[sink].add(moved)
    labels = jnp.searchsorted(jnp.cumsum(tallies), jnp.arange(rows * top), side="right").astype(jnp.int32)
    table = labels.reshape(top, rows).T
    table = table[jax.random.permutation(jax.random.fold_in(own, 1), rows)]
    offset_by = jax.random.randint(jax.random.fold_in(own, 2), (rows, 1), 0, top)
    return jnp.take_along_axis(table, (jnp.arange(top)[None, :] + offset_by) % top, axis=1)


def load_shares(amount, total, bound, slope, full):
    weights = [(1 << 20) // math.isqrt(standing ** slope) + 1 for standing in range(1, amount + 1)]
    largest = bound if full else min(bound, max(-(-total // amount), total * weights[0] // sum(weights)))
    least = 1 if total - largest >= amount - 1 else 0
    holding, spare = [largest] + [least] * (amount - 1), total - largest - least * (amount - 1)
    while spare > 0:
        movable = [i for i in range(1, amount) if holding[i] < largest] or [i for i in range(1, amount) if holding[i] < bound]
        whole, budget = sum([weights[i] for i in movable]), spare
        for i in movable:
            addition = min(bound - holding[i], max(1, budget * weights[i] // whole), spare)
            holding[i] = holding[i] + addition
            spare = spare - addition
    return np.array(holding)


def scatter_about(own_key, extent, deviation, bound, shards=(), kind=jnp.bfloat16):
    gain = level_of(own_key, extent, shards, -0.22, 0.18) if shards else 1.0
    entries = jax.random.normal(own_key, extent, jnp.float32) * deviation * gain
    return jnp.minimum(jnp.maximum(entries, -bound), bound).astype(kind)


def setup_inputs(seed: int = 0) -> dict:
    key_of = jax.random.split(jax.random.key(seed), 7)
    tokens = scatter_about(key_of[0], (TOKENS, D), 1.0, 6.0, ((0, 256),))
    expert_ids_keys = jax.random.split(jax.random.fold_in(key_of[1], 1), TOKENS // TOK_DEV)
    expert_ids_turns = jax.random.permutation(jax.random.fold_in(key_of[1], 3), TOKENS // TOK_DEV)
    expert_ids = jax.vmap(lambda own, number: assign_block(jax.random.fold_in(key_of[1], 2), own, number, TOK_DEV, EXPERTS, TOP, CAP, 2))(expert_ids_keys, expert_ids_turns).reshape((TOKENS, TOP))
    gate_quota = set_ends(jax.random.randint(key_of[2], (TOKENS, TOP), 1, 32768), jax.random.fold_in(key_of[2], 1), 1, 32767).astype(jnp.int32)
    w_gate = scatter_about(key_of[3], (EXPERTS * GROUP, D, FF // GROUP), D ** -0.5, 0.09375, ((0, 32), (2, 8)))
    w_up = scatter_about(key_of[4], (EXPERTS * GROUP, D, FF // GROUP), D ** -0.5, 0.09375, ((0, 32), (2, 8)))
    w_down = scatter_about(key_of[5], (EXPERTS * GROUP, FF // GROUP, D), FF ** -0.5, 0.0625, ((0, 32), (1, 8)))
    return {"tokens": tokens, "expert_ids": expert_ids, "gate_quota": gate_quota, "w_gate": w_gate, "w_up": w_up, "w_down": w_down}


def reference(tokens, expert_ids, gate_quota, w_gate, w_up, w_down):
    col_count = FF // GROUP
    block_count = GROUP * N_DP
    block_width = FF // block_count
    gate_all = w_gate.reshape(EXPERTS, GROUP, D, col_count).transpose(0, 2, 1, 3).reshape(EXPERTS, D, FF)
    up_all = w_up.reshape(EXPERTS, GROUP, D, col_count).transpose(0, 2, 1, 3).reshape(EXPERTS, D, FF)
    down_all = w_down.reshape(EXPERTS, FF, D)
    flat_ids = expert_ids.reshape(-1)
    most_rows = CAP * N_DP * N_EXPERT
    per_assign = jnp.zeros((TOKENS * TOP, D), jnp.float32)

    def add_block(running, operands):
        term = jnp.dot(operands[0], operands[1], preferred_element_type=jnp.float32).astype(jnp.bfloat16)
        term = lax.optimization_barrier(term)
        return running + term.astype(jnp.float32), None

    for expert in range(EXPERTS):
        picked = flat_ids == expert
        chosen = jnp.nonzero(picked, size=most_rows, fill_value=0)[0].astype(jnp.int32)
        is_valid = (jnp.arange(most_rows, dtype=jnp.int32) < jnp.sum(picked.astype(jnp.int32))).astype(jnp.float32)
        expert_rows = tokens[chosen // TOP]
        gate_act = jnp.dot(expert_rows, gate_all[expert], preferred_element_type=jnp.float32)
        up_act = jnp.dot(expert_rows, up_all[expert], preferred_element_type=jnp.float32)
        hidden = (jax.nn.silu(gate_act) * up_act).astype(jnp.bfloat16)
        hidden_blocks = hidden.reshape(most_rows, block_count, block_width).transpose(1, 0, 2)
        down_blocks = down_all[expert].reshape(block_count, block_width, D)
        out_rows, _ = lax.scan(add_block, jnp.zeros((most_rows, D), jnp.float32), (hidden_blocks, down_blocks))
        per_assign = per_assign.at[chosen].add(out_rows * is_valid[:, None])
    quota = gate_quota.astype(jnp.float32)
    shares = quota / jnp.sum(quota, axis=1, keepdims=True)
    mixed_out = jnp.sum(per_assign.reshape(TOKENS, TOP, D) * shares[:, :, None], axis=1)
    return mixed_out.astype(jnp.bfloat16)
```

```python
import functools

import jax
import jax.numpy as jnp
from jax import lax
from jax.experimental import pallas as pl
from jax.experimental.pallas import tpu as pltpu
from jax.sharding import Mesh, PartitionSpec as P

EXPERTS = 8
TOP = 2
CAP = 6
NX, NH, NL, NY, NC = 4, 2, 4, 4, 2
HALF = NX * CAP
AXES = ("y", "c", "x", "h", "l")
Z = ("h", "l")
YC = ("y", "c")
STEPS = 4


def ring_pairs():
    return [
        (y * NC + c, ((y + (1 if c == 0 else -1)) % NY) * NC + c)
        for y in range(NY)
        for c in range(NC)
    ]


def around_y(v):
    return lax.ppermute(v, YC, ring_pairs())


def across_z(v, m):
    return lax.ppermute(v, Z, [(z, z ^ m) for z in range(NH * NL)])


def along_x(v, k):
    return lax.ppermute(v, "x", [(i, (i + k) % NX) for i in range(NX)])


def swap_cores(v):
    return lax.ppermute(v, "c", [(0, 1), (1, 0)])


def ffn_body(r0, r1, r2, r3, g0, g1, u0, u1, d0, d1, o0, o1, o2, o3, x_s, acc_s, hid_s):
    i = pl.program_id(0)
    rows = r0.shape[0]

    @pl.when(i < STEPS)
    def _():
        for k, r in enumerate((r0, r1, r2, r3)):
            x_s[k * rows : (k + 1) * rows, :] = r[...]
        x = x_s[...]
        for k, w in enumerate((g0, g1, u0, u1)):
            p = jnp.dot(x, w[0], preferred_element_type=jnp.float32)
            acc_s[k] = jnp.where(i == 0, p, acc_s[k] + p)

    @pl.when(i == STEPS - 1)
    def _():
        for k in range(2):
            hid_s[k] = (jax.nn.silu(acc_s[k]) * acc_s[2 + k]).astype(jnp.bfloat16)

    @pl.when(i >= STEPS)
    def _():
        out = jnp.dot(hid_s[0], d0[0], preferred_element_type=jnp.float32)
        out += jnp.dot(hid_s[1], d1[0], preferred_element_type=jnp.float32)
        out = out.astype(jnp.bfloat16)
        for k, o in enumerate((o0, o1, o2, o3)):
            o[...] = out[k * rows : (k + 1) * rows, :]


def ffn(pieces, g, u, d):
    rows, width = pieces[0].shape
    hid = g[0].shape[2]
    kb = width // STEPS
    up = lambda i: (0, jnp.minimum(i, STEPS - 1), 0)
    down = lambda i: (0, 0, jnp.maximum(i - STEPS, 0))
    total = NY * rows
    return pl.pallas_call(
        ffn_body,
        grid=(2 * STEPS,),
        in_specs=[pl.BlockSpec((rows, kb), lambda i: (0, jnp.minimum(i, STEPS - 1)))] * NY
        + [pl.BlockSpec((1, kb, hid), up)] * 4
        + [pl.BlockSpec((1, hid, kb), down)] * 2,
        out_specs=[pl.BlockSpec((rows, kb), lambda i: (0, jnp.maximum(i - STEPS, 0)))] * NY,
        out_shape=[jax.ShapeDtypeStruct((rows, width), jnp.bfloat16)] * NY,
        scratch_shapes=[
            pltpu.VMEM((total, kb), jnp.bfloat16),
            pltpu.VMEM((4, total, hid), jnp.float32),
            pltpu.VMEM((2, total, hid), jnp.bfloat16),
        ],
        compiler_params=pltpu.CompilerParams(
            dimension_semantics=("arbitrary",), vmem_limit_bytes=40 * 1024 * 1024
        ),
        cost_estimate=pl.CostEstimate(
            flops=2 * 3 * total * width * 2 * hid,
            bytes_accessed=12 * width * hid + 4 * total * width,
            transcendentals=total * 2 * hid,
        ),
        name="ffn",
    )(*pieces, g[0], g[1], u[0], u[1], d[0], d[1])


def add(a, b):
    return (a.astype(jnp.float32) + b.astype(jnp.float32)).astype(jnp.bfloat16)


def on_device(tokens, expert_ids, gate_quota, w_gate, w_up, w_down):
    tok_rows = tokens.shape[0]
    x = lax.axis_index("x")
    h = lax.axis_index("h")
    slots = EXPERTS * CAP
    g = (w_gate, swap_cores(w_gate))
    u = (w_up, swap_cores(w_up))
    d = (w_down, swap_cores(w_down))

    hit = expert_ids[:, :, None] == jnp.arange(EXPERTS, dtype=jnp.int32)
    hit_f = hit.astype(jnp.float32)
    named = jnp.sum(hit_f, axis=1)
    before = jnp.tril(jnp.ones((tok_rows, tok_rows), jnp.float32), -1)
    earlier = jnp.dot(before, named, preferred_element_type=jnp.float32)
    position = jnp.sum(earlier[:, None, :] * hit_f, axis=2).astype(jnp.int32)
    slot = ((expert_ids // 2 - x) % NX) * (2 * CAP) + ((expert_ids % 2) ^ h) * CAP + position
    at = slot[:, :, None] == jnp.arange(slots, dtype=jnp.int32)
    placing = jnp.sum(at.astype(jnp.float32), axis=1).astype(jnp.bfloat16)
    packed = lax.dot_general(
        placing, tokens, (((0,), (0,)), ((), ())), preferred_element_type=jnp.float32
    ).astype(jnp.bfloat16)

    two = 2 * CAP
    cols = [packed[:two]] + [along_x(packed[k * two : (k + 1) * two], k) for k in range(1, NX)]
    own = jnp.concatenate([c[:CAP] for c in cols])
    other = jnp.concatenate([c[CAP:] for c in cols])
    got = {0: own}
    for m in (7, 1, 6, 2, 5, 3, 4):
        got[m] = across_z(own if m < NL else other, m)

    outs = []
    for j in range(NL):
        piece = jnp.concatenate([got[j], got[7 - j]])
        pieces = [piece]
        for _ in range(NY - 1):
            piece = around_y(piece)
            pieces.append(piece)
        outs.append(ffn(pieces, g, u, d))

    back = {}
    for j in (1, 2, 3, 0):
        o = outs[j]
        r = around_y(o[1])
        r = around_y(add(o[2], r))
        r = around_y(add(o[3], r))
        lo = add(o[0][:HALF], r[:HALF])
        hi = add(o[0][HALF:], r[HALF:])
        back[j] = across_z(lo, j) if j else lo
        back[7 - j] = across_z(hi, 7 - j)

    f32 = lambda v: v.astype(jnp.float32)
    own_sum = ((f32(back[0]) + f32(back[1])) + (f32(back[2]) + f32(back[3]))).astype(jnp.bfloat16)
    other_sum = ((f32(back[4]) + f32(back[5])) + (f32(back[6]) + f32(back[7]))).astype(jnp.bfloat16)
    home = []
    for k in range(NX):
        part = jnp.concatenate([own_sum[k * CAP : (k + 1) * CAP], other_sum[k * CAP : (k + 1) * CAP]])
        home.append(along_x(part, -k) if k else part)
    expert_out = jnp.concatenate(home)

    quota = gate_quota.astype(jnp.float32)
    shares = quota / jnp.sum(quota, axis=1, keepdims=True)
    mixing = jnp.sum(at.astype(jnp.float32) * shares[:, :, None], axis=1)
    mixed = jnp.dot(
        mixing,
        expert_out.astype(jnp.float32),
        preferred_element_type=jnp.float32,
        precision=lax.Precision.HIGHEST,
    )
    return mixed.astype(jnp.bfloat16)


def solution(mesh):
    split = Mesh(mesh.devices.reshape(NY, NC, NX, NH, NL), AXES)
    rows = P(AXES, None)
    return jax.shard_map(
        on_device,
        mesh=split,
        in_specs=(
            rows,
            rows,
            rows,
            P(("x", "h", "l"), None, YC),
            P(("x", "h", "l"), None, YC),
            P(("x", "h", "l"), YC, None),
        ),
        out_specs=rows,
        check_vma=False,
    )
```
